32 devices in a mesh: ctx: 4 (over x, core), seq: 8 (over z, y).
Axes of the slice: x: 2, y: 2, z: 4, core: 2. Of those that a mesh axis runs over, the one named last changes fastest.
Arguments:
- queries: bfloat16 [6144, 1024], P(('seq', 'ctx')), parts along dimension 0, may hold values from -6 to 6
- key_vectors: bfloat16 [6144, 128], P(('seq', 'ctx')), parts along dimension 0, may hold values from -4 to 4
- value_vectors: bfloat16 [6144, 128], P(('seq', 'ctx')), parts along dimension 0, may hold values from -6 to 6
- out_grad: bfloat16 [6144, 1024], P(('seq', 'ctx')), parts along dimension 0, may hold values from -6 to 6
- span_order: int32 [64], P('seq'), parts along dimension 0, may hold values from 0 to 7, each once
- doc_lengths: int32 [48], P('seq'), parts along dimension 0, may hold values from 1 to 256, 768 in all
Outputs:
- attended: bfloat16 [6144, 1024], P(('seq', 'ctx')), parts along dimension 0
- query_grad: bfloat16 [6144, 1024], P(('seq', 'ctx')), parts along dimension 0
- key_grad: bfloat16 [6144, 128], P(('seq', 'ctx')), parts along dimension 0
- value_grad: bfloat16 [6144, 128], P(('seq', 'ctx')), parts along dimension 0
The draws below stay inside these ranges and needn't reach their ends.
There are 8 independent parts, one for each index of `seq`. The reference program is written for one: setup_inputs(seed, part) draws one part's arguments, and reference() takes and returns one part's arrays. A program takes and returns all parts, laid end to end along the dimension named above; each array names one. Nothing has to cross between parts.
Inputs may be any that keep to these rules, and one draw needn't show every extreme that they name: `span_order`: each of 0 to 7 appears once. `doc_lengths`: the lengths sum to 768.
All inputs are finite; a program needn't handle non-finite values.
Results may differ from the reference program's by a relative error of at most 0.015.
Values may be sent and summed in bfloat16 or wider, within the bound.
No kernel may reach another device: no remote copies, remote signals or barrier semaphores. Data moves between devices by JAX's collectives and lax.ppermute only.
A program may use at most 64 MiB of HBM per device.

```python
import math
import jax
import jax.numpy as jnp
import numpy as np
from jax import lax

HQ = 8
DH = 128
TOK_DEV = 192
DOCS = 6
SPAN = 96
NCH = 8
SEQ = 768
DOC_MOST = 256
N_CTX = 4


def draw_queries(key, part):
    own_key = jax.random.fold_in(key, 11)
    base = jnp.clip(jax.random.normal(own_key, (SEQ, HQ * DH), jnp.float32), -4.0, 4.0)
    return base.astype(jnp.bfloat16)


def draw_key_vectors(key, part):
    own_key = jax.random.fold_in(key, 13)
    base = jnp.clip(jax.random.normal(own_key, (SEQ, DH), jnp.float32), -4.0, 4.0)
    return base.astype(jnp.bfloat16)


def block_scale(rng, shape, split, least, top_value):
    loudness = 1.0
    for position, shards_of in split:
        draws = jax.random.uniform(jax.random.fold_in(jax.random.fold_in(rng, 6), position), (shards_of,), jnp.float32, least / len(split), top_value / len(split))
        loudness = loudness * jnp.repeat(jnp.exp(draws), shape[position] // shards_of).reshape((-1,) + (1,) * (len(shape) - 1 - position))
    return loudness


def profile(count, total, bound, lean):
    loads = [(1 << 20) // math.isqrt(standing ** lean) + 1 for standing in range(2, count + 1)]
    spare, holding = total - bound - (count - 1), [1] * (count - 1)
    while spare > 0:
        movable = [i for i in range(count - 1) if holding[i] < bound]
        pool, remaining = sum([loads[i] for i in movable]), spare
        for i in movable:
            more = min(bound - holding[i], max(1, remaining * loads[i] // pool), spare)
            holding[i] = holding[i] + more
            spare = spare - more
    return np.array([bound] + holding)


def uneven_parts(key, amount, total, reach, skew):
    if amount == 2:
        one = jax.random.randint(key, (), max(1, total - reach), min(reach, total - 1) + 1)
        return jnp.stack([one, total - one])
    lengths = jnp.asarray(profile(amount, total, reach, skew), jnp.int32)
    couples = (amount - 1) // 2
    donor, taker = lengths[1:1 + 2 * couples:2], lengths[2:2 + 2 * couples:2]
    room = jnp.minimum(donor - 1, reach - taker)
    shifted = jax.random.randint(jax.random.fold_in(key, 1), (couples,), 0, 1 << 20) % (room + 1)
    lengths = lengths.at[1:1 + 2 * couples:2].set(donor - shifted).at[2:2 + 2 * couples:2].set(taker + shifted)
    return lengths[jax.random.permutation(jax.random.fold_in(key, 2), amount)]


def normal_values(stream_key, dims, width, reach, cuts=(), kind=jnp.bfloat16):
    values = width * jax.random.normal(stream_key, dims, jnp.float32)
    if cuts:
        values = values * block_scale(stream_key, dims, cuts, -0.22, 0.18)
    return jnp.clip(values, -reach, reach).astype(kind)


def setup_inputs(seed: int = 0, part: int = 0) -> dict:
    key_of = jax.random.split(jax.random.key(seed), 7)
    part_keys = jax.random.split(jax.random.fold_in(key_of[6], part), 7)
    return {
        "queries": draw_queries(jax.random.fold_in(jax.random.fold_in(key_of[6], part), 71), part),
        "key_vectors": draw_key_vectors(jax.random.fold_in(jax.random.fold_in(key_of[6], part), 71), part),
        "value_vectors": normal_values(part_keys[2], (SEQ, DH), 1.0, 6.0, ((0, 4),)),
        "out_grad": normal_values(part_keys[3], (SEQ, HQ * DH), 1.0, 6.0, ((0, 4),)),
        "span_order": jax.random.permutation(part_keys[4], NCH).astype(jnp.int32),
        "doc_lengths": uneven_parts(part_keys[5], DOCS, SEQ, DOC_MOST, 2).astype(jnp.int32),
    }


negative_fill = -1e+30

def rounded(values_in):
    return lax.optimization_barrier(values_in.astype(jnp.bfloat16)).astype(jnp.float32)

def layout(span_order, doc_lengths):
    offsets = jnp.arange(SPAN, dtype=jnp.int32)
    positions = (span_order.astype(jnp.int32)[:, None] * SPAN + offsets[None, :]).reshape(SEQ)
    doc_ends = jnp.cumsum(doc_lengths).astype(jnp.int32)
    documents = lax.optimization_barrier(jnp.sum((positions[:, None] >= doc_ends[None, :]).astype(jnp.int32), axis=1))
    return (positions, documents)

def reference(queries, key_vectors, value_vectors, out_grad, span_order, doc_lengths):
    score_scale = 1.0 / math.sqrt(DH)
    positions, documents = layout(span_order, doc_lengths)
    key_float = key_vectors.astype(jnp.float32)
    value_float = value_vectors.astype(jnp.float32)

    def query_block(running, block_index):
        key_sum, value_sum = running
        first_row = (block_index * TOK_DEV).astype(jnp.int32)
        query_heads = lax.dynamic_slice_in_dim(queries, first_row, TOK_DEV, 0).astype(jnp.float32).reshape(TOK_DEV, HQ, DH)
        grad_heads = lax.dynamic_slice_in_dim(out_grad, first_row, TOK_DEV, 0).astype(jnp.float32).reshape(TOK_DEV, HQ, DH)
        query_pos = lax.dynamic_slice_in_dim(positions, first_row, TOK_DEV, 0)
        query_doc = lax.dynamic_slice_in_dim(documents, first_row, TOK_DEV, 0)
        allowed = ((query_doc[:, None] == documents[None, :]) & (positions[None, :] <= query_pos[:, None]))[:, None, :]
        scores = jnp.einsum('rhd,kd->rhk', query_heads, key_float) * score_scale
        row_max = lax.optimization_barrier(jnp.max(jnp.where(allowed, scores, negative_fill), axis=-1, keepdims=True))
        weights = jnp.where(allowed, jnp.exp(scores - row_max), 0.0)
        row_sum = lax.optimization_barrier(jnp.sum(weights, axis=-1, keepdims=True))
        attended = (jnp.einsum('rhk,kd->rhd', rounded(weights), value_float) / row_sum).astype(jnp.bfloat16)
        log_norm = row_max + jnp.log(row_sum)
        out_float = lax.optimization_barrier(attended).astype(jnp.float32)
        row_dots = lax.optimization_barrier(jnp.sum(grad_heads * out_float, axis=-1, keepdims=True))
        back_weights = jnp.where(allowed, jnp.exp(scores - log_norm), 0.0)
        value_part = jnp.einsum('rhk,rhd->kd', rounded(back_weights), grad_heads)
        weight_grads = jnp.einsum('rhd,kd->rhk', grad_heads, value_float)
        score_grads = rounded(back_weights * (weight_grads - row_dots))
        query_grad = (jnp.einsum('rhk,kd->rhd', score_grads, key_float) * score_scale).astype(jnp.bfloat16)
        key_part = jnp.einsum('rhk,rhd->kd', score_grads, query_heads)
        return ((key_sum + key_part, value_sum + value_part), (attended.reshape(TOK_DEV, HQ * DH), query_grad.reshape(TOK_DEV, HQ * DH)))
    zeros = jnp.zeros((SEQ, DH), jnp.float32)
    totals, outputs = lax.scan(query_block, (zeros, zeros), jnp.arange(N_CTX, dtype=jnp.int32))
    key_sum, value_sum = totals
    attended, query_grad = outputs
    return (attended.reshape(SEQ, HQ * DH), query_grad.reshape(SEQ, HQ * DH), (key_sum * score_scale).astype(jnp.bfloat16), value_sum.astype(jnp.bfloat16))
```

```python
import math

import jax
import jax.numpy as jnp
from jax import lax
from jax.experimental import pallas as pl
from jax.experimental.pallas import tpu as pltpu
from jax.sharding import PartitionSpec as P

DH = 128
TILE = 384
FILL = -1e30

NT = (((1,), (1,)), ((), ()))
NN = (((1,), (0,)), ((), ()))
TN = (((0,), (0,)), ((), ()))


def mm(a, b, dims):
    return lax.dot_general(a, b, dims, preferred_element_type=jnp.float32)


def attention_kernel(n, heads, span, spans_all, docs, so, dl, own_ref, *refs):
    spans_own = spans_all // n
    tok = span * spans_own
    rows = heads * span
    scale = 1.0 / math.sqrt(DH)
    grow = scale * math.log2(math.e)
    q_ref, g_ref = refs[0], refs[1]
    kv = refs[2 : 2 + n]
    outs = refs[2 + n :]
    att_ref, dq_ref = outs[0], outs[1]
    parts = outs[2 : 2 + n]
    ks, vs, dk, dv, qs, gs, bias, sc, dp, pb, db, mx, ls, dd, oa, qa = outs[2 + n :]
    pad = TILE
    own = own_ref[0]

    def place(slot):
        return pl.multiple_of(so[slot] * span + pad, 16)

    ks[0:pad, :] = jnp.zeros((pad, DH), ks.dtype)
    vs[0:pad, :] = jnp.zeros((pad, DH), vs.dtype)
    dk[...] = jnp.zeros(dk.shape, dk.dtype)
    dv[...] = jnp.zeros(dv.shape, dv.dtype)
    for m in range(n):
        base = (own ^ m) * spans_own
        for j in range(spans_own):
            at = place(base + j)
            ks[pl.ds(at, span), :] = kv[m][j * span : (j + 1) * span, 0:DH]
            vs[pl.ds(at, span), :] = kv[m][j * span : (j + 1) * span, DH : 2 * DH]

    for j in range(spans_own):
        first = so[own * spans_own + j] * span
        stop = first + span
        edge = jnp.int32(0)
        begin = jnp.int32(0)
        pos = first + lax.broadcasted_iota(jnp.int32, (span, TILE), 0)
        begin_row = jnp.zeros((span, TILE), jnp.int32)
        for d in range(docs):
            edge = edge + dl[d]
            begin = jnp.where(edge <= first, edge, begin)
            begin_row = jnp.where(edge <= pos, edge, begin_row)
        count = (stop - begin + TILE - 1) // TILE
        lane = lax.broadcasted_iota(jnp.int32, (span, TILE), 1)
        for h in range(heads):
            at = slice(h * span, (h + 1) * span)
            qs[at, :] = q_ref[j * span : (j + 1) * span, h * DH : (h + 1) * DH]
            gs[at, :] = g_ref[j * span : (j + 1) * span, h * DH : (h + 1) * DH]

        def tile_at(t):
            return pl.multiple_of(stop + pad - (t + 1) * TILE, 16)

        def bias_of(t):
            key_pos = lane + (stop - (t + 1) * TILE)
            return jnp.where((key_pos <= pos) & (key_pos >= begin_row), 0.0, FILL)

        def finish(t, h, e, grads, inv, mean):
            at = slice(h * span, (h + 1) * span)
            p = e * inv
            pb[at, :] = p.astype(jnp.bfloat16)
            db[at, :] = (p * (grads - mean)).astype(jnp.bfloat16)

        def products(t):
            start = tile_at(t)
            kt = ks[pl.ds(start, TILE), :]
            vt = vs[pl.ds(start, TILE), :]
            p = pb[...]
            d = db[...]
            dv[pl.ds(start, TILE), :] += mm(p, gs[...], TN)
            dk[pl.ds(start, TILE), :] += mm(d, qs[...], TN)
            return mm(p, vt, NN), mm(d, kt, NN)

        def store(o, dq):
            for h in range(heads):
                at = slice(h * span, (h + 1) * span)
                to = (slice(j * span, (j + 1) * span), slice(h * DH, (h + 1) * DH))
                att_ref[to] = o[at, :].astype(att_ref.dtype)
                dq_ref[to] = (dq[at, :] * scale).astype(dq_ref.dtype)

        @pl.when(count == 1)
        def _():
            start = tile_at(0)
            kt = ks[pl.ds(start, TILE), :]
            vt = vs[pl.ds(start, TILE), :]
            bias[...] = bias_of(0)
            sc[0] = mm(qs[...], kt, NT)
            dp[0] = mm(gs[...], vt, NT)
            for h in range(heads):
                at = slice(h * span, (h + 1) * span)
                s = sc[0, at, :] + bias[...]
                e = jnp.exp2((s - jnp.max(s, axis=1, keepdims=True)) * grow)
                grads = dp[0, at, :]
                inv = 1.0 / jnp.sum(e, axis=1, keepdims=True)
                mean = jnp.sum(e * grads, axis=1, keepdims=True) * inv
                finish(0, h, e, grads, inv, mean)
            store(*products(0))

        @pl.when(count > 1)
        def _():
            mx[...] = jnp.full(mx.shape, FILL, mx.dtype)
            ls[...] = jnp.zeros(ls.shape, ls.dtype)
            dd[...] = jnp.zeros(dd.shape, dd.dtype)
            oa[...] = jnp.zeros(oa.shape, oa.dtype)
            qa[...] = jnp.zeros(qa.shape, qa.dtype)

            def first_pass(t, c):
                start = tile_at(t)
                bias[...] = bias_of(t)
                s_all = mm(qs[...], ks[pl.ds(start, TILE), :], NT)
                dp[t] = mm(gs[...], vs[pl.ds(start, TILE), :], NT)
                for h in range(heads):
                    at = slice(h * span, (h + 1) * span)
                    s = s_all[at, :] + bias[...]
                    sc[t, at, :] = s
                    mx[at, :] = jnp.maximum(mx[at, :], jnp.max(s, axis=1, keepdims=True))
                return c

            def second_pass(t, c):
                for h in range(heads):
                    at = slice(h * span, (h + 1) * span)
                    e = jnp.exp2((sc[t, at, :] - mx[at, 0:1]) * grow)
                    sc[t, at, :] = e
                    ls[at, :] += jnp.sum(e, axis=1, keepdims=True)
                    dd[at, :] += jnp.sum(e * dp[t, at, :], axis=1, keepdims=True)
                return c

            def third_pass(t, c):
                for h in range(heads):
                    at = slice(h * span, (h + 1) * span)
                    inv = 1.0 / ls[at, 0:1]
                    finish(t, h, sc[t, at, :], dp[t, at, :], inv, dd[at, 0:1] * inv)
                o, dq = products(t)
                oa[...] += o
                qa[...] += dq
                return c

            lax.fori_loop(0, count, first_pass, 0)
            lax.fori_loop(0, count, second_pass, 0)
            lax.fori_loop(0, count, third_pass, 0)
            store(oa[...], qa[...])

    for m in range(n):
        base = (own ^ m) * spans_own
        for j in range(spans_own):
            at = place(base + j)
            to = slice(j * span, (j + 1) * span)
            parts[m][to, 0:DH] = (dk[pl.ds(at, span), :] * scale).astype(parts[m].dtype)
            parts[m][to, DH : 2 * DH] = dv[pl.ds(at, span), :].astype(parts[m].dtype)


def local(queries, key_vectors, value_vectors, out_grad, span_order, doc_lengths):
    tok, width = queries.shape
    n = lax.axis_size("ctx")
    heads = width // DH
    spans_all = span_order.shape[0]
    docs = doc_lengths.shape[0]
    seq = tok * n
    span = seq // spans_all
    rows = heads * span
    tiles = -(-seq // TILE)
    own = lax.axis_index("ctx").astype(jnp.int32).reshape(1)

    def swap(x, m):
        return lax.ppermute(x, "ctx", [(i, i ^ m) for i in range(n)])

    both = jnp.concatenate([key_vectors, value_vectors], axis=1)
    kv = [both] + [swap(both, m) for m in range(1, n)]

    vm = pl.BlockSpec(memory_space=pltpu.VMEM)
    sm = pl.BlockSpec(memory_space=pltpu.SMEM)
    bf, f32 = jnp.bfloat16, jnp.float32
    out_shape = [
        jax.ShapeDtypeStruct((tok, width), bf),
        jax.ShapeDtypeStruct((tok, width), bf),
        jax.ShapeDtypeStruct((tok, 2 * DH), f32),
    ] + [jax.ShapeDtypeStruct((tok, 2 * DH), bf)] * (n - 1)
    V = pltpu.VMEM
    scratch = [
        V((TILE + seq, DH), bf),
        V((TILE + seq, DH), bf),
        V((TILE + seq, DH), f32),
        V((TILE + seq, DH), f32),
        V((rows, DH), bf),
        V((rows, DH), bf),
        V((span, TILE), f32),
        V((tiles, rows, TILE), f32),
        V((tiles, rows, TILE), f32),
        V((rows, TILE), bf),
        V((rows, TILE), bf),
        V((rows, DH), f32),
        V((rows, DH), f32),
        V((rows, DH), f32),
        V((rows, DH), f32),
        V((rows, DH), f32),
    ]

    def body(*refs):
        attention_kernel(n, heads, span, spans_all, docs, *refs)

    res = pl.pallas_call(
        body,
        out_shape=out_shape,
        in_specs=[sm, sm, sm] + [vm] * (2 + n),
        out_specs=[vm] * len(out_shape),
        scratch_shapes=scratch,
        compiler_params=pltpu.CompilerParams(vmem_limit_bytes=(16 + 3 * tiles) << 20),
        name="attention",
    )(span_order, doc_lengths, own, queries, out_grad, *kv)
    got = [swap(res[2 + m], m) for m in range(1, n)]

    def merge(own_ref, *refs):
        total = own_ref[...]
        for ref in refs[:-2]:
            total = total + ref[...].astype(f32)
        refs[-2][...] = total[:, :DH].astype(bf)
        refs[-1][...] = total[:, DH:].astype(bf)

    half = jax.ShapeDtypeStruct((tok, DH), bf)
    key_grad, value_grad = pl.pallas_call(
        merge,
        out_shape=[half, half],
        in_specs=[vm] * n,
        out_specs=[vm, vm],
        compiler_params=pltpu.CompilerParams(vmem_limit_bytes=4 << 20),
        name="merge",
    )(res[2], *got)
    return res[0], res[1], key_grad, value_grad


def solution(mesh):
    rows = P(("seq", "ctx"), None)
    return jax.shard_map(
        local,
        mesh=mesh,
        in_specs=(rows, rows, rows, rows, P("seq"), P("seq")),
        out_specs=(rows, rows, rows, rows),
        check_vma=False,
    )
```

```python
import math

import jax
import jax.numpy as jnp
from jax import lax
from jax.experimental import pallas as pl
from jax.experimental.pallas import tpu as pltpu
from jax.sharding import PartitionSpec as P

DH = 128
TILE = 384
FILL = -1e30
SCALE = 1.0 / math.sqrt(DH)
GROW = SCALE * math.log2(math.e)

NT = (((1,), (1,)), ((), ()))
NN = (((1,), (0,)), ((), ()))
TN = (((0,), (0,)), ((), ()))


def mm(a, b, dims):
    return lax.dot_general(a, b, dims, preferred_element_type=jnp.float32)


def window(so, dl, slot, span, docs):
    first = so[slot] * span
    stop = first + span
    edge = jnp.int32(0)
    begin = jnp.int32(0)
    for d in range(docs):
        edge = edge + dl[d]
        begin = jnp.where(edge <= first, edge, begin)
    return first, stop, (stop - begin + TILE - 1) // TILE


def plan(meta, n, span, spans_all, docs):
    own = lax.axis_index("ctx")
    spans_own = spans_all // n
    dl = [meta[spans_all + d] for d in range(docs)]
    wins = [window(meta, dl, own * spans_own + j, span, docs) for j in range(spans_own)]
    short = wins[0][2] == 1
    for w in wins[1:]:
        short = short & (w[2] == 1)
    return own, dl, wins, short


def prepare_kernel(n, heads, span, spans_all, docs, meta, both, qs, gs, bias):
    own, dl, wins, short = plan(meta, n, span, spans_all, docs)
    tok = len(wins) * span
    for j, (first, stop, count) in enumerate(wins):
        for h in range(heads):
            to = slice(h * span, (h + 1) * span)
            cols = slice(h * DH, (h + 1) * DH)
            qs[j, to, :] = both[j * span : (j + 1) * span, cols]
            gs[j, to, :] = both[tok + j * span : tok + (j + 1) * span, cols]
        bias[j] = bias_tile(dl, docs, span, first, stop)


def bias_tile(dl, docs, span, first, tile_stop):
    pos = first + lax.broadcasted_iota(jnp.int32, (span, TILE), 0)
    edge = jnp.int32(0)
    begin_row = jnp.zeros((span, TILE), jnp.int32)
    for d in range(docs):
        edge = edge + dl[d]
        begin_row = jnp.where(edge <= pos, edge, begin_row)
    key_pos = lax.broadcasted_iota(jnp.int32, (span, TILE), 1) + (tile_stop - TILE)
    return jnp.where((key_pos <= pos) & (key_pos >= begin_row), 0.0, FILL)


def front_kernel(n, heads, span, spans_all, docs, meta, qs, gs, bias, *refs):
    own, dl, wins, short = plan(meta, n, span, spans_all, docs)
    spans_own = spans_all // n
    kv = refs[0:n]
    parts = refs[n : 2 * n]
    pb, db, kw, vw, oa, qa = refs[2 * n : 2 * n + 6]
    ks, vs, dk, dv, sc, dp, mx, ls, dd, more = refs[2 * n + 6 :]
    pad = TILE
    head_rows = [slice(h * span, (h + 1) * span) for h in range(heads)]
    ks[0:pad, :] = jnp.zeros((pad, DH), ks.dtype)
    vs[0:pad, :] = jnp.zeros((pad, DH), vs.dtype)
    dk[...] = jnp.zeros(dk.shape, dk.dtype)
    dv[...] = jnp.zeros(dv.shape, dv.dtype)

    def place(m, j):
        return pl.multiple_of(meta[(own ^ m) * spans_own + j] * span + pad, 16)

    for m in range(n):
        for j in range(spans_own):
            at = place(m, j)
            ks[pl.ds(at, span), :] = kv[m][j * span : (j + 1) * span, 0:DH]
            vs[pl.ds(at, span), :] = kv[m][j * span : (j + 1) * span, DH : 2 * DH]

    def tile_at(j, t):
        return pl.multiple_of(wins[j][1] + pad - (t + 1) * TILE, 16)

    def finish(j, h, e, grads, inv, mean):
        p = e * inv
        pb[j, head_rows[h], :] = p.astype(jnp.bfloat16)
        db[j, head_rows[h], :] = (p * (grads - mean)).astype(jnp.bfloat16)

    def key_side(j, t):
        start = tile_at(j, t)
        dv[pl.ds(start, TILE), :] += mm(pb[j], gs[j], TN)
        dk[pl.ds(start, TILE), :] += mm(db[j], qs[j], TN)

    @pl.when(short)
    def _():
        for j in range(spans_own):
            start = tile_at(j, 0)
            kw[j] = ks[pl.ds(start, TILE), :]
            vw[j] = vs[pl.ds(start, TILE), :]
        for j in range(spans_own):
            sc[j] = mm(qs[j], kw[j], NT)
            dp[j] = mm(gs[j], vw[j], NT)
            for h in range(heads):
                s = sc[j, head_rows[h], :] + bias[j]
                e = jnp.exp2((s - jnp.max(s, axis=1, keepdims=True)) * GROW)
                grads = dp[j, head_rows[h], :]
                inv = 1.0 / jnp.sum(e, axis=1, keepdims=True)
                mean = jnp.sum(e * grads, axis=1, keepdims=True) * inv
                finish(j, h, e, grads, inv, mean)
        for j in range(spans_own):
            key_side(j, 0)

    @pl.when(jnp.logical_not(short))
    def _():
        for j in range(spans_own):
            mx[...] = jnp.full(mx.shape, FILL, mx.dtype)
            ls[...] = jnp.zeros(ls.shape, ls.dtype)
            dd[...] = jnp.zeros(dd.shape, dd.dtype)
            oa[j] = jnp.zeros(oa.shape[1:], oa.dtype)
            qa[j] = jnp.zeros(qa.shape[1:], qa.dtype)

            def first_pass(t, c):
                start = tile_at(j, t)
                more[...] = bias_tile(dl, docs, span, wins[j][0], wins[j][1] - t * TILE)
                dp[t] = mm(qs[j], ks[pl.ds(start, TILE), :], NT)
                for at in head_rows:
                    s = dp[t, at, :] + more[...]
                    sc[t, at, :] = s
                    mx[at, :] = jnp.maximum(mx[at, :], jnp.max(s, axis=1, keepdims=True))
                dp[t] = mm(gs[j], vs[pl.ds(start, TILE), :], NT)
                return c

            def second_pass(t, c):
                for at in head_rows:
                    e = jnp.exp2((sc[t, at, :] - mx[at, 0:1]) * GROW)
                    sc[t, at, :] = e
                    ls[at, :] += jnp.sum(e, axis=1, keepdims=True)
                    dd[at, :] += jnp.sum(e * dp[t, at, :], axis=1, keepdims=True)
                return c

            def third_pass(t, c):
                start = tile_at(j, t)
                for h in range(heads):
                    at = head_rows[h]
                    inv = 1.0 / ls[at, 0:1]
                    finish(j, h, sc[t, at, :], dp[t, at, :], inv, dd[at, 0:1] * inv)
                key_side(j, t)
                oa[j] += mm(pb[j], vs[pl.ds(start, TILE), :], NN)
                qa[j] += mm(db[j], ks[pl.ds(start, TILE), :], NN)
                return c

            count = wins[j][2]
            lax.fori_loop(0, count, first_pass, 0)
            lax.fori_loop(0, count, second_pass, 0)
            lax.fori_loop(0, count, third_pass, 0)

    for m in range(n):
        for j in range(spans_own):
            at = place(m, j)
            to = slice(j * span, (j + 1) * span)
            parts[m][to, 0:DH] = (dk[pl.ds(at, span), :] * SCALE).astype(parts[m].dtype)
            parts[m][to, DH : 2 * DH] = dv[pl.ds(at, span), :].astype(parts[m].dtype)


def back_kernel(n, heads, span, spans_all, docs, meta, *refs):
    pb, db, kw, vw, oa, qa, att_ref, dq_ref = refs
    own, dl, wins, short = plan(meta, n, span, spans_all, docs)
    spans_own = len(wins)

    def store(j, o, dq):
        for h in range(heads):
            at = slice(h * span, (h + 1) * span)
            to = (slice(j * span, (j + 1) * span), slice(h * DH, (h + 1) * DH))
            att_ref[to] = o[at, :].astype(att_ref.dtype)
            dq_ref[to] = (dq[at, :] * SCALE).astype(dq_ref.dtype)

    @pl.when(short)
    def _():
        for j in range(spans_own):
            store(j, mm(pb[j], vw[j], NN), mm(db[j], kw[j], NN))

    @pl.when(jnp.logical_not(short))
    def _():
        for j in range(spans_own):
            store(j, oa[j], qa[j])


def merge_kernel(a, b, c, key_ref, value_ref):
    total = a[...].astype(jnp.float32) + b[...].astype(jnp.float32) + c[...].astype(jnp.float32)
    key_ref[...] = total[:, :DH].astype(key_ref.dtype)
    value_ref[...] = total[:, DH:].astype(value_ref.dtype)


def local(queries, key_vectors, value_vectors, out_grad, span_order, doc_lengths):
    tok, width = queries.shape
    n = lax.axis_size("ctx")
    heads = width // DH
    spans_all = span_order.shape[0]
    spans_own = spans_all // n
    docs = doc_lengths.shape[0]
    seq = tok * n
    span = seq // spans_all
    rows = heads * span
    tiles = max(spans_own, -(-seq // TILE))
    bits = [1 << b for b in range(n.bit_length() - 1)]
    bf, f32 = jnp.bfloat16, jnp.float32

    def swap(x, m):
        return lax.ppermute(x, "ctx", [(i, i ^ m) for i in range(n)])

    vm = pl.BlockSpec(memory_space=pltpu.VMEM)
    sm = pl.BlockSpec(memory_space=pltpu.SMEM)
    S = jax.ShapeDtypeStruct
    V = pltpu.VMEM
    sizes = (n, heads, span, spans_all, docs)

    def prepare(*refs):
        prepare_kernel(*sizes, *refs)

    def front(*refs):
        front_kernel(*sizes, *refs)

    def back(*refs):
        back_kernel(*sizes, *refs)

    part = [S((tok, 2 * DH), bf if m % 2 else f32) for m in range(n)]
    middle = [
        S((spans_own, rows, TILE), bf),
        S((spans_own, rows, TILE), bf),
        S((spans_own, TILE, DH), bf),
        S((spans_own, TILE, DH), bf),
        S((spans_own, rows, DH), f32),
        S((spans_own, rows, DH), f32),
    ]
    def side(a, b, axis):
        before = [(0, 0)] * a.ndim
        after = [(0, 0)] * a.ndim
        before[axis] = (a.shape[axis], 0)
        after[axis] = (0, b.shape[axis])
        return jnp.pad(a, after) + jnp.pad(b, before)

    kv = {0: side(key_vectors, value_vectors, 1)}
    meta = side(span_order, doc_lengths, 0)
    for bit in reversed(bits):
        for m in list(kv):
            with jax.named_scope("hop%d" % bit):
                kv[m | bit] = swap(kv[m], bit)
    qs, gs, bias = pl.pallas_call(
        prepare,
        out_shape=[
            S((spans_own, rows, DH), bf),
            S((spans_own, rows, DH), bf),
            S((spans_own, span, TILE), f32),
        ],
        in_specs=[sm, vm],
        out_specs=[vm, vm, vm],
        compiler_params=pltpu.CompilerParams(vmem_limit_bytes=8 << 20),
        name="prepare",
    )(meta, side(queries, out_grad, 0))
    res = pl.pallas_call(
        front,
        out_shape=part + middle,
        in_specs=[sm] + [vm] * (3 + n),
        out_specs=[vm] * (n + 6),
        scratch_shapes=[
            V((TILE + seq, DH), bf),
            V((TILE + seq, DH), bf),
            V((TILE + seq, DH), f32),
            V((TILE + seq, DH), f32),
            V((tiles, rows, TILE), f32),
            V((tiles, rows, TILE), f32),
            V((rows, DH), f32),
            V((rows, DH), f32),
            V((rows, DH), f32),
            V((span, TILE), f32),
        ],
        compiler_params=pltpu.CompilerParams(vmem_limit_bytes=(16 + 3 * tiles) << 20),
        name="front",
    )(meta, qs, gs, bias, *[kv[m] for m in range(n)])
    attended, query_grad = pl.pallas_call(
        back,
        out_shape=[S((tok, width), bf), S((tok, width), bf)],
        in_specs=[sm] + [vm] * 6,
        out_specs=[vm, vm],
        compiler_params=pltpu.CompilerParams(vmem_limit_bytes=16 << 20),
        name="back",
    )(meta, *res[n:])

    held = {m: [res[m]] for m in range(n)}
    for bit in bits:
        for m in sorted(held, reverse=True):
            if m & bit:
                mine = held.pop(m)
                block = mine[0].astype(f32)
                for other in mine[1:]:
                    block = block + other.astype(f32)
                held[m ^ bit].append(swap(block.astype(bf), bit))
    terms = held[0]
    while len(terms) > 3:
        terms = [terms[0].astype(f32) + terms[1].astype(f32)] + terms[2:]
    half = S((tok, DH), bf)
    key_grad, value_grad = pl.pallas_call(
        merge_kernel,
        out_shape=[half, half],
        in_specs=[vm] * 3,
        out_specs=[vm, vm],
        compiler_params=pltpu.CompilerParams(vmem_limit_bytes=4 << 20),
        name="merge",
    )(*terms)
    return attended, query_grad, key_grad, value_grad


def solution(mesh):
    rows = P(("seq", "ctx"), None)
    return jax.shard_map(
        local,
        mesh=mesh,
        in_specs=(rows, rows, rows, rows, P("seq"), P("seq")),
        out_specs=(rows, rows, rows, rows),
        check_vma=False,
    )
```

```python
import math

import jax
import jax.numpy as jnp
from jax import lax
from jax.experimental import pallas as pl
from jax.experimental.pallas import tpu as pltpu
from jax.sharding import PartitionSpec as P

DH = 128
TILE = 384
BLOCK = 16
FILL = -1e30
SCALE = 1.0 / math.sqrt(DH)
GROW = SCALE * math.log2(math.e)

NT = (((1,), (1,)), ((), ()))
NN = (((1,), (0,)), ((), ()))
TN = (((0,), (0,)), ((), ()))


def mm(a, b, dims):
    return lax.dot_general(a, b, dims, preferred_element_type=jnp.float32)


def window(so, dl, slot, span, docs):
    first = so[slot] * span
    stop = first + span
    edge = jnp.int32(0)
    begin = jnp.int32(0)
    for d in range(docs):
        edge = edge + dl[d]
        begin = jnp.where(edge <= first, edge, begin)
    return first, stop, (stop - begin + TILE - 1) // TILE


def unpack(info, n, span, spans_all, docs):
    spans_own = spans_all // n
    at = [info[0, i] for i in range(spans_all)]
    stops = [info[0, spans_all + j] for j in range(spans_own)]
    counts = [info[0, spans_all + spans_own + j] for j in range(spans_own)]
    short = counts[0] == 1
    for c in counts[1:]:
        short = short & (c == 1)
    wins = [(stop - span, stop, count) for stop, count in zip(stops, counts)]
    return at, wins, short


def prepare_kernel(n, heads, span, spans_all, docs, meta, both, qs, gs, bias, info, qt, gt):
    own = lax.axis_index("ctx")
    spans_own = spans_all // n
    dl = [meta[spans_all + d] for d in range(docs)]
    wins = [window(meta, dl, own * spans_own + j, span, docs) for j in range(spans_own)]
    tok = spans_own * span
    values = [
        meta[(own ^ m) * spans_own + j] * span + TILE for m in range(n) for j in range(spans_own)
    ]
    values += [w[1] for w in wins] + [w[2] for w in wins] + dl
    lane = lax.broadcasted_iota(jnp.int32, info.shape, 1)
    packed = jnp.zeros(info.shape, jnp.int32)
    for i, value in enumerate(values):
        packed = jnp.where(lane == i, value, packed)
    info[...] = packed
    for j, (first, stop, count) in enumerate(wins):
        for h in range(heads):
            to = slice(h * span, (h + 1) * span)
            cols = slice(h * DH, (h + 1) * DH)
            qs[j, to, :] = both[j * span : (j + 1) * span, cols]
            gs[j, to, :] = both[tok + j * span : tok + (j + 1) * span, cols]
        bias[j] = bias_tile(dl, docs, span, first, stop)
        qt[j] = qs[j].T
        gt[j] = gs[j].T


def bias_tile(dl, docs, span, first, tile_stop):
    pos = first + lax.broadcasted_iota(jnp.int32, (span, TILE), 0)
    edge = jnp.int32(0)
    begin_row = jnp.zeros((span, TILE), jnp.int32)
    for d in range(docs):
        edge = edge + dl[d]
        begin_row = jnp.where(edge <= pos, edge, begin_row)
    key_pos = lax.broadcasted_iota(jnp.int32, (span, TILE), 1) + (tile_stop - TILE)
    return jnp.where((key_pos <= pos) & (key_pos >= begin_row), 0.0, FILL)


def front_kernel(n, heads, span, spans_all, docs, info, qs, gs, bias, qt, gt, *refs):
    spots, wins, short = unpack(info, n, span, spans_all, docs)
    spans_own = spans_all // n
    kv = refs[0:n]
    parts = refs[n : 2 * n]
    pb, db, kw, vw, oa, qa = refs[2 * n : 2 * n + 6]
    ks, vs, dk, dv, sc, dp, mx, ls, dd, more = refs[2 * n + 6 :]
    pad = TILE
    head_rows = [slice(h * span, (h + 1) * span) for h in range(heads)]
    ks[0:pad, :] = jnp.zeros((pad, DH), ks.dtype)
    vs[0:pad, :] = jnp.zeros((pad, DH), vs.dtype)
    dk[...] = jnp.zeros(dk.shape, dk.dtype)
    dv[...] = jnp.zeros(dv.shape, dv.dtype)

    def place(m, j):
        return pl.multiple_of(spots[m * spans_own + j], 16)

    for m in range(n):
        for j in range(spans_own):
            at = place(m, j)
            ks[pl.ds(at, span), :] = kv[m][j * span : (j + 1) * span, 0:DH]
            vs[pl.ds(at, span), :] = kv[m][j * span : (j + 1) * span, DH : 2 * DH]

    def tile_at(j, t):
        return pl.multiple_of(wins[j][1] + pad - (t + 1) * TILE, 16)

    def finish(j, at, e, grads, inv, mean):
        p = e * inv
        pb[j, at, :] = p.astype(jnp.bfloat16)
        db[j, at, :] = (p * (grads - mean)).astype(jnp.bfloat16)

    def key_side(j, t):
        start = tile_at(j, t)
        dv[pl.ds(start, TILE), :] += mm(gt[j], pb[j], NN).T
        dk[pl.ds(start, TILE), :] += mm(qt[j], db[j], NN).T

    @pl.when(short)
    def _():
        for j in range(spans_own):
            start = tile_at(j, 0)
            kw[j] = ks[pl.ds(start, TILE), :]
            vw[j] = vs[pl.ds(start, TILE), :]
        for j in range(spans_own):
            sc[j] = mm(qs[j], kw[j], NT)
            dp[j] = mm(gs[j], vw[j], NT)
            for r in range(0, heads * span, BLOCK):
                at = slice(r, r + BLOCK)
                s = sc[j, at, :] + bias[j, r % span : r % span + BLOCK, :]
                e = jnp.exp2((s - jnp.max(s, axis=1, keepdims=True)) * GROW)
                grads = dp[j, at, :]
                inv = 1.0 / jnp.sum(e, axis=1, keepdims=True)
                mean = jnp.sum(e * grads, axis=1, keepdims=True) * inv
                finish(j, at, e, grads, inv, mean)
        for j in range(spans_own):
            key_side(j, 0)

    @pl.when(jnp.logical_not(short))
    def _():
        dl = [info[0, spans_all + 2 * spans_own + d] for d in range(docs)]
        for j in range(spans_own):
            mx[...] = jnp.full(mx.shape, FILL, mx.dtype)
            ls[...] = jnp.zeros(ls.shape, ls.dtype)
            dd[...] = jnp.zeros(dd.shape, dd.dtype)
            oa[j] = jnp.zeros(oa.shape[1:], oa.dtype)
            qa[j] = jnp.zeros(qa.shape[1:], qa.dtype)

            def first_pass(t, c):
                start = tile_at(j, t)
                more[...] = bias_tile(dl, docs, span, wins[j][0], wins[j][1] - t * TILE)
                dp[t] = mm(qs[j], ks[pl.ds(start, TILE), :], NT)
                for at in head_rows:
                    s = dp[t, at, :] + more[...]
                    sc[t, at, :] = s
                    mx[at, :] = jnp.maximum(mx[at, :], jnp.max(s, axis=1, keepdims=True))
                dp[t] = mm(gs[j], vs[pl.ds(start, TILE), :], NT)
                return c

            def second_pass(t, c):
                for at in head_rows:
                    e = jnp.exp2((sc[t, at, :] - mx[at, 0:1]) * GROW)
                    sc[t, at, :] = e
                    ls[at, :] += jnp.sum(e, axis=1, keepdims=True)
                    dd[at, :] += jnp.sum(e * dp[t, at, :], axis=1, keepdims=True)
                return c

            def third_pass(t, c):
                start = tile_at(j, t)
                for at in head_rows:
                    inv = 1.0 / ls[at, 0:1]
                    finish(j, at, sc[t, at, :], dp[t, at, :], inv, dd[at, 0:1] * inv)
                key_side(j, t)
                oa[j] += mm(pb[j], vs[pl.ds(start, TILE), :], NN)
                qa[j] += mm(db[j], ks[pl.ds(start, TILE), :], NN)
                return c

            count = wins[j][2]
            lax.fori_loop(0, count, first_pass, 0)
            lax.fori_loop(0, count, second_pass, 0)
            lax.fori_loop(0, count, third_pass, 0)

    for m in range(n):
        for j in range(spans_own):
            at = place(m, j)
            to = slice(j * span, (j + 1) * span)
            parts[m][to, 0:DH] = (dk[pl.ds(at, span), :] * SCALE).astype(parts[m].dtype)
            parts[m][to, DH : 2 * DH] = dv[pl.ds(at, span), :].astype(parts[m].dtype)


def back_kernel(n, heads, span, spans_all, docs, info, *refs):
    pb, db, kw, vw, oa, qa, att_ref, dq_ref = refs
    unused, wins, short = unpack(info, n, span, spans_all, docs)
    spans_own = len(wins)

    def store(j, o, dq):
        for h in range(heads):
            at = slice(h * span, (h + 1) * span)
            to = (slice(j * span, (j + 1) * span), slice(h * DH, (h + 1) * DH))
            att_ref[to] = o[at, :].astype(att_ref.dtype)
            dq_ref[to] = (dq[at, :] * SCALE).astype(dq_ref.dtype)

    @pl.when(short)
    def _():
        for j in range(spans_own):
            store(j, mm(pb[j], vw[j], NN), mm(db[j], kw[j], NN))

    @pl.when(jnp.logical_not(short))
    def _():
        for j in range(spans_own):
            store(j, oa[j], qa[j])


def merge_kernel(a, b, c, key_ref, value_ref):
    total = a[...].astype(jnp.float32) + b[...].astype(jnp.float32) + c[...].astype(jnp.float32)
    key_ref[...] = total[:, :DH].astype(key_ref.dtype)
    value_ref[...] = total[:, DH:].astype(value_ref.dtype)


def local(queries, key_vectors, value_vectors, out_grad, span_order, doc_lengths):
    tok, width = queries.shape
    n = lax.axis_size("ctx")
    heads = width // DH
    spans_all = span_order.shape[0]
    spans_own = spans_all // n
    docs = doc_lengths.shape[0]
    seq = tok * n
    span = seq // spans_all
    rows = heads * span
    tiles = max(spans_own, -(-seq // TILE))
    bits = [1 << b for b in range(n.bit_length() - 1)]
    bf, f32 = jnp.bfloat16, jnp.float32

    def swap(x, m):
        return lax.ppermute(x, "ctx", [(i, i ^ m) for i in range(n)])

    vm = pl.BlockSpec(memory_space=pltpu.VMEM)
    sm = pl.BlockSpec(memory_space=pltpu.SMEM)
    S = jax.ShapeDtypeStruct
    V = pltpu.VMEM
    sizes = (n, heads, span, spans_all, docs)

    def prepare(*refs):
        prepare_kernel(*sizes, *refs)

    def front(*refs):
        front_kernel(*sizes, *refs)

    def back(*refs):
        back_kernel(*sizes, *refs)

    part = [S((tok, 2 * DH), bf if m % 2 else f32) for m in range(n)]
    middle = [
        S((spans_own, rows, TILE), bf),
        S((spans_own, rows, TILE), bf),
        S((spans_own, TILE, DH), bf),
        S((spans_own, TILE, DH), bf),
        S((spans_own, rows, DH), f32),
        S((spans_own, rows, DH), f32),
    ]
    def side(a, b, axis):
        before = [(0, 0)] * a.ndim
        after = [(0, 0)] * a.ndim
        before[axis] = (a.shape[axis], 0)
        after[axis] = (0, b.shape[axis])
        return jnp.pad(a, after) + jnp.pad(b, before)

    kv = {0: side(key_vectors, value_vectors, 1)}
    meta = side(span_order, doc_lengths, 0)
    for bit in reversed(bits):
        for m in list(kv):
            with jax.named_scope("hop%d" % bit):
                kv[m | bit] = swap(kv[m], bit)
    qs, gs, bias, info, qt, gt = pl.pallas_call(
        prepare,
        out_shape=[
            S((spans_own, rows, DH), bf),
            S((spans_own, rows, DH), bf),
            S((spans_own, span, TILE), f32),
            S((8, 128 * -(-(spans_all + 2 * spans_own + docs) // 128)), jnp.int32),
            S((spans_own, DH, rows), bf),
            S((spans_own, DH, rows), bf),
        ],
        in_specs=[sm, vm],
        out_specs=[vm] * 6,
        compiler_params=pltpu.CompilerParams(vmem_limit_bytes=8 << 20),
        name="prepare",
    )(meta, side(queries, out_grad, 0))
    res = pl.pallas_call(
        front,
        out_shape=part + middle,
        in_specs=[vm] * (6 + n),
        out_specs=[vm] * (n + 6),
        scratch_shapes=[
            V((TILE + seq, DH), bf),
            V((TILE + seq, DH), bf),
            V((TILE + seq, DH), f32),
            V((TILE + seq, DH), f32),
            V((tiles, rows, TILE), f32),
            V((tiles, rows, TILE), f32),
            V((rows, DH), f32),
            V((rows, DH), f32),
            V((rows, DH), f32),
            V((span, TILE), f32),
        ],
        compiler_params=pltpu.CompilerParams(vmem_limit_bytes=(16 + 3 * tiles) << 20),
        name="front",
    )(info, qs, gs, bias, qt, gt, *[kv[m] for m in range(n)])
    attended, query_grad = pl.pallas_call(
        back,
        out_shape=[S((tok, width), bf), S((tok, width), bf)],
        in_specs=[vm] * 7,
        out_specs=[vm, vm],
        compiler_params=pltpu.CompilerParams(vmem_limit_bytes=16 << 20),
        name="back",
    )(info, *res[n:])

    held = {m: [res[m]] for m in range(n)}
    for bit in bits:
        for m in sorted(held, reverse=True):
            if m & bit:
                mine = held.pop(m)
                block = mine[0].astype(f32)
                for other in mine[1:]:
                    block = block + other.astype(f32)
                held[m ^ bit].append(swap(block.astype(bf), bit))
    terms = held[0]
    while len(terms) > 3:
        terms = [terms[0].astype(f32) + terms[1].astype(f32)] + terms[2:]
    half = S((tok, DH), bf)
    key_grad, value_grad = pl.pallas_call(
        merge_kernel,
        out_shape=[half, half],
        in_specs=[vm] * 3,
        out_specs=[vm, vm],
        compiler_params=pltpu.CompilerParams(vmem_limit_bytes=4 << 20),
        name="merge",
    )(*terms)
    return attended, query_grad, key_grad, value_grad


def solution(mesh):
    rows = P(("seq", "ctx"), None)
    return jax.shard_map(
        local,
        mesh=mesh,
        in_specs=(rows, rows, rows, rows, P("seq"), P("seq")),
        out_specs=(rows, rows, rows, rows),
        check_vma=False,
    )
```

```python
import math

import jax
import jax.numpy as jnp
from jax import lax
from jax.experimental import pallas as pl
from jax.experimental.pallas import tpu as pltpu
from jax.sharding import PartitionSpec as P

DH = 128
TILE = 384
BLOCK = 16
FILL = -1e30
SCALE = 1.0 / math.sqrt(DH)
GROW = SCALE * math.log2(math.e)

NT = (((1,), (1,)), ((), ()))
NN = (((1,), (0,)), ((), ()))
TN = (((0,), (0,)), ((), ()))


def mm(a, b, dims):
    return lax.dot_general(a, b, dims, preferred_element_type=jnp.float32)


def window(so, dl, slot, span, docs):
    first = so[slot] * span
    stop = first + span
    edge = jnp.int32(0)
    begin = jnp.int32(0)
    for d in range(docs):
        edge = edge + dl[d]
        begin = jnp.where(edge <= first, edge, begin)
    return first, stop, (stop - begin + TILE - 1) // TILE


def unpack(info, n, span, spans_all, docs):
    spans_own = spans_all // n
    at = [info[0, i] for i in range(spans_all)]
    stops = [info[0, spans_all + j] for j in range(spans_own)]
    counts = [info[0, spans_all + spans_own + j] for j in range(spans_own)]
    short = counts[0] == 1
    for c in counts[1:]:
        short = short & (c == 1)
    wins = [(stop - span, stop, count) for stop, count in zip(stops, counts)]
    return at, wins, short


def prepare_kernel(n, heads, span, spans_all, docs, meta, both, qs, gs, mask, info, qt, gt, dk, dv):
    own = lax.axis_index("ctx")
    spans_own = spans_all // n
    dl = [meta[spans_all + d] for d in range(docs)]
    wins = [window(meta, dl, own * spans_own + j, span, docs) for j in range(spans_own)]
    tok = spans_own * span
    values = [
        meta[(own ^ m) * spans_own + j] * span + TILE for m in range(n) for j in range(spans_own)
    ]
    values += [w[1] for w in wins] + [w[2] for w in wins] + dl
    lane = lax.broadcasted_iota(jnp.int32, info.shape, 1)
    packed = jnp.zeros(info.shape, jnp.int32)
    for i, value in enumerate(values):
        packed = jnp.where(lane == i, value, packed)
    info[...] = packed
    wide = qs.shape[2] - DH
    row = lax.broadcasted_iota(jnp.int32, (span, wide), 0)
    unit = (row == lax.broadcasted_iota(jnp.int32, (span, wide), 1)).astype(jnp.float32).astype(qs.dtype)
    for j, (first, stop, count) in enumerate(wins):
        for h in range(heads):
            to = slice(h * span, (h + 1) * span)
            cols = slice(h * DH, (h + 1) * DH)
            qs[j, to, 0:DH] = both[j * span : (j + 1) * span, cols]
            gs[j, to, :] = both[tok + j * span : tok + (j + 1) * span, cols]
            qs[j, to, DH:] = unit
        qt[j] = qs[j, :, 0:DH].T
        gt[j] = gs[j].T
        mask[j] = tile_mask(dl, first, stop - TILE, mask.shape[1:], 1).astype(mask.dtype)
    dk[...] = jnp.zeros(dk.shape, dk.dtype)
    dv[...] = jnp.zeros(dv.shape, dv.dtype)


def tile_mask(dl, first, low, shape, row_axis):
    pos = first + lax.broadcasted_iota(jnp.int32, shape, row_axis)
    key_pos = low + lax.broadcasted_iota(jnp.int32, shape, 1 - row_axis)
    edge = jnp.int32(0)
    begin_row = jnp.zeros(shape, jnp.int32)
    for length in dl:
        edge = edge + length
        begin_row = jnp.where(edge <= pos, edge, begin_row)
    return jnp.where((key_pos <= pos) & (key_pos >= begin_row), 0.0, FILL)


def front_kernel(n, heads, span, spans_all, docs, info, qs, gs, mask, qt, gt, zk, zv, *refs):
    spots, wins, short = unpack(info, n, span, spans_all, docs)
    spans_own = spans_all // n
    kv = refs[0:n]
    parts = refs[n : 2 * n - 1]
    pb, db, kw, vw, oa, qa, dk, dv = refs[2 * n - 1 : 2 * n + 7]
    ks, vs, sc, dp, mx, ls, dd, more = refs[2 * n + 7 :]
    pad = TILE
    head_rows = [slice(h * span, (h + 1) * span) for h in range(heads)]
    ks[0:pad, :] = jnp.zeros((pad, DH), ks.dtype)
    vs[0:pad, :] = jnp.zeros((pad, DH), vs.dtype)

    def place(m, j):
        return pl.multiple_of(spots[m * spans_own + j], 16)

    for m in range(n):
        for j in range(spans_own):
            at = place(m, j)
            ks[pl.ds(at, span), :] = kv[m][j * span : (j + 1) * span, 0:DH]
            vs[pl.ds(at, span), :] = kv[m][j * span : (j + 1) * span, DH : 2 * DH]

    def tile_at(j, t):
        return pl.multiple_of(wins[j][1] + pad - (t + 1) * TILE, 16)

    def finish(j, at, e, grads, inv, mean):
        p = e * inv
        pb[j, at, :] = p.astype(jnp.bfloat16)
        db[j, at, :] = (p * (grads - mean)).astype(jnp.bfloat16)

    def key_side(j, t):
        start = tile_at(j, t)
        dv[pl.ds(start, TILE), :] += mm(gt[j], pb[j], NN).T
        dk[pl.ds(start, TILE), :] += mm(qt[j], db[j], NN).T

    @pl.when(short)
    def _():
        for j in range(spans_own):
            start = tile_at(j, 0)
            kw[j, :, 0:DH] = ks[pl.ds(start, TILE), :]
            kw[j, :, DH:] = mask[j]
            vw[j] = vs[pl.ds(start, TILE), :]
        for j in range(spans_own):
            sc[j] = mm(qs[j], kw[j], NT)
            dp[j] = mm(gs[j], vw[j], NT)
            for r in range(0, heads * span, BLOCK):
                at = slice(r, r + BLOCK)
                s = sc[j, at, :]
                e = jnp.exp2((s - jnp.max(s, axis=1, keepdims=True)) * GROW)
                grads = dp[j, at, :]
                inv = 1.0 / jnp.sum(e, axis=1, keepdims=True)
                mean = jnp.sum(e * grads, axis=1, keepdims=True) * inv
                finish(j, at, e, grads, inv, mean)
        for j in range(spans_own):
            key_side(j, 0)

    @pl.when(jnp.logical_not(short))
    def _():
        dl = [info[0, spans_all + 2 * spans_own + d] for d in range(docs)]
        for j in range(spans_own):
            mx[...] = jnp.full(mx.shape, FILL, mx.dtype)
            ls[...] = jnp.zeros(ls.shape, ls.dtype)
            dd[...] = jnp.zeros(dd.shape, dd.dtype)
            oa[j] = jnp.zeros(oa.shape[1:], oa.dtype)
            qa[j] = jnp.zeros(qa.shape[1:], qa.dtype)

            def first_pass(t, c):
                start = tile_at(j, t)
                more[...] = tile_mask(dl, wins[j][0], wins[j][1] - (t + 1) * TILE, more.shape, 0)
                dp[t] = mm(qs[j, :, 0:DH], ks[pl.ds(start, TILE), :], NT)
                for at in head_rows:
                    s = dp[t, at, :] + more[...]
                    sc[t, at, :] = s
                    mx[at, :] = jnp.maximum(mx[at, :], jnp.max(s, axis=1, keepdims=True))
                dp[t] = mm(gs[j], vs[pl.ds(start, TILE), :], NT)
                return c

            def second_pass(t, c):
                for at in head_rows:
                    e = jnp.exp2((sc[t, at, :] - mx[at, 0:1]) * GROW)
                    sc[t, at, :] = e
                    ls[at, :] += jnp.sum(e, axis=1, keepdims=True)
                    dd[at, :] += jnp.sum(e * dp[t, at, :], axis=1, keepdims=True)
                return c

            def third_pass(t, c):
                start = tile_at(j, t)
                for at in head_rows:
                    inv = 1.0 / ls[at, 0:1]
                    finish(j, at, sc[t, at, :], dp[t, at, :], inv, dd[at, 0:1] * inv)
                key_side(j, t)
                oa[j] += mm(pb[j], vs[pl.ds(start, TILE), :], NN)
                qa[j] += mm(db[j], ks[pl.ds(start, TILE), :], NN)
                return c

            count = wins[j][2]
            lax.fori_loop(0, count, first_pass, 0)
            lax.fori_loop(0, count, second_pass, 0)
            lax.fori_loop(0, count, third_pass, 0)

    for m in range(1, n):
        for j in range(spans_own):
            take_block(parts[m - 1], dk, dv, place(m, j), j, span)


def take_block(out, dk, dv, at, j, span):
    to = slice(j * span, (j + 1) * span)
    out[to, 0:DH] = (dk[pl.ds(at, span), :] * SCALE).astype(out.dtype)
    out[to, DH : 2 * DH] = dv[pl.ds(at, span), :].astype(out.dtype)


def back_kernel(n, heads, span, spans_all, docs, info, *refs):
    pb, db, kw, vw, oa, qa, dk, dv, att_ref, dq_ref, mine = refs
    spots, wins, short = unpack(info, n, span, spans_all, docs)
    spans_own = len(wins)

    def store(j, o, dq):
        for h in range(heads):
            at = slice(h * span, (h + 1) * span)
            to = (slice(j * span, (j + 1) * span), slice(h * DH, (h + 1) * DH))
            att_ref[to] = o[at, :].astype(att_ref.dtype)
            dq_ref[to] = (dq[at, :] * SCALE).astype(dq_ref.dtype)

    @pl.when(short)
    def _():
        for j in range(spans_own):
            store(j, mm(pb[j], vw[j], NN), mm(db[j], kw[j, :, 0:DH], NN))

    @pl.when(jnp.logical_not(short))
    def _():
        for j in range(spans_own):
            store(j, oa[j], qa[j])

    for j in range(spans_own):
        take_block(mine, dk, dv, pl.multiple_of(spots[j], 16), j, span)


def merge_kernel(a, b, c, key_ref, value_ref):
    total = a[...].astype(jnp.float32) + b[...].astype(jnp.float32) + c[...].astype(jnp.float32)
    key_ref[...] = total[:, :DH].astype(key_ref.dtype)
    value_ref[...] = total[:, DH:].astype(value_ref.dtype)


def local(queries, key_vectors, value_vectors, out_grad, span_order, doc_lengths):
    tok, width = queries.shape
    n = lax.axis_size("ctx")
    heads = width // DH
    spans_all = span_order.shape[0]
    spans_own = spans_all // n
    docs = doc_lengths.shape[0]
    seq = tok * n
    span = seq // spans_all
    rows = heads * span
    lanes = DH + 128 * (-(-span // 128))
    tiles = max(spans_own, -(-seq // TILE))
    bits = [1 << b for b in range(n.bit_length() - 1)]
    bf, f32 = jnp.bfloat16, jnp.float32

    def swap(x, m):
        return lax.ppermute(x, "ctx", [(i, i ^ m) for i in range(n)])

    vm = pl.BlockSpec(memory_space=pltpu.VMEM)
    sm = pl.BlockSpec(memory_space=pltpu.SMEM)
    S = jax.ShapeDtypeStruct
    V = pltpu.VMEM
    sizes = (n, heads, span, spans_all, docs)

    def prepare(*refs):
        prepare_kernel(*sizes, *refs)

    def front(*refs):
        front_kernel(*sizes, *refs)

    def back(*refs):
        back_kernel(*sizes, *refs)

    part = [S((tok, 2 * DH), bf if m % 2 else f32) for m in range(1, n)]
    middle = [
        S((spans_own, rows, TILE), bf),
        S((spans_own, rows, TILE), bf),
        S((spans_own, TILE, lanes), bf),
        S((spans_own, TILE, DH), bf),
        S((spans_own, rows, DH), f32),
        S((spans_own, rows, DH), f32),
        S((TILE + seq, DH), f32),
        S((TILE + seq, DH), f32),
    ]
    def side(a, b, axis):
        before = [(0, 0)] * a.ndim
        after = [(0, 0)] * a.ndim
        before[axis] = (a.shape[axis], 0)
        after[axis] = (0, b.shape[axis])
        return jnp.pad(a, after) + jnp.pad(b, before)

    kv = {0: side(key_vectors, value_vectors, 1)}
    meta = side(span_order, doc_lengths, 0)
    for bit in reversed(bits):
        for m in list(kv):
            with jax.named_scope("hop%d" % bit):
                kv[m | bit] = swap(kv[m], bit)
    qs, gs, mask, info, qt, gt, zk, zv = pl.pallas_call(
        prepare,
        out_shape=[
            S((spans_own, rows, lanes), bf),
            S((spans_own, rows, DH), bf),
            S((spans_own, TILE, lanes - DH), bf),
            S((8, 128 * -(-(spans_all + 2 * spans_own + docs) // 128)), jnp.int32),
            S((spans_own, DH, rows), bf),
            S((spans_own, DH, rows), bf),
            S((TILE + seq, DH), f32),
            S((TILE + seq, DH), f32),
        ],
        in_specs=[sm, vm],
        out_specs=[vm] * 8,
        compiler_params=pltpu.CompilerParams(vmem_limit_bytes=8 << 20),
        name="prepare",
    )(meta, side(queries, out_grad, 0))
    res = pl.pallas_call(
        front,
        out_shape=part + middle,
        in_specs=[vm] * (8 + n),
        out_specs=[vm] * (n + 7),
        input_output_aliases={6: n + 5, 7: n + 6},
        scratch_shapes=[
            V((TILE + seq, DH), bf),
            V((TILE + seq, DH), bf),
            V((tiles, rows, TILE), f32),
            V((tiles, rows, TILE), f32),
            V((rows, DH), f32),
            V((rows, DH), f32),
            V((rows, DH), f32),
            V((span, TILE), f32),
        ],
        compiler_params=pltpu.CompilerParams(vmem_limit_bytes=(16 + 3 * tiles) << 20),
        name="front",
    )(info, qs, gs, mask, qt, gt, zk, zv, *[kv[m] for m in range(n)])
    attended, query_grad, mine = pl.pallas_call(
        back,
        out_shape=[S((tok, width), bf), S((tok, width), bf), S((tok, 2 * DH), f32)],
        in_specs=[vm] * 9,
        out_specs=[vm] * 3,
        compiler_params=pltpu.CompilerParams(vmem_limit_bytes=16 << 20),
        name="back",
    )(info, *res[n - 1 :])

    held = {0: [mine]}
    for m in range(1, n):
        held[m] = [res[m - 1]]
    for bit in bits:
        for m in sorted(held, reverse=True):
            if m & bit:
                mine = held.pop(m)
                block = mine[0].astype(f32)
                for other in mine[1:]:
                    block = block + other.astype(f32)
                held[m ^ bit].append(swap(block.astype(bf), bit))
    terms = held[0]
    while len(terms) > 3:
        terms = [terms[0].astype(f32) + terms[1].astype(f32)] + terms[2:]
    half = S((tok, DH), bf)
    key_grad, value_grad = pl.pallas_call(
        merge_kernel,
        out_shape=[half, half],
        in_specs=[vm] * 3,
        out_specs=[vm, vm],
        compiler_params=pltpu.CompilerParams(vmem_limit_bytes=4 << 20),
        name="merge",
    )(*terms)
    return attended, query_grad, key_grad, value_grad


def solution(mesh):
    rows = P(("seq", "ctx"), None)
    return jax.shard_map(
        local,
        mesh=mesh,
        in_specs=(rows, rows, rows, rows, P("seq"), P("seq")),
        out_specs=(rows, rows, rows, rows),
        check_vma=False,
    )
```
